512 devices in a mesh: dp: 8 (over z), ctx: 4 (over y_lo, core), tp: 16 (over y_hi, x).
Axes of the slice: x: 4, y: 8 (y_hi: 4, y_lo: 2; y = y_hi * 2 + y_lo), z: 8, core: 2. Of those that a mesh axis runs over, the one named last changes fastest.
Arguments:
- layer_input: bfloat16 [8, 1024, 8192], P('dp', ('ctx', 'tp')), may hold values from -6 to 6
- value_weight: bfloat16 [8192, 4096], P(('dp', 'ctx'), 'tp'), may hold values from -0.0625 to 0.0625
- query_raw: bfloat16 [8, 1024, 4096], P('dp', 'ctx', 'tp'), may hold values from -6 to 6
- key_raw: bfloat16 [8, 1024, 4096], P('dp', 'ctx', 'tp'), may hold values from -6 to 6
- out_grad: bfloat16 [8, 1024, 4096], P('dp', 'ctx', 'tp'), may hold values from -6 to 6
- gate_logits: float32 [2, 8, 32, 1024], P(None, 'dp', 'tp', 'ctx'), may hold values from -14 to 4, as said below
- decay_params: float32 [2, 32], P(None, 'tp'), may hold values from -0.35 to 0.35
- saved_states: float32 [8, 4, 32, 128, 128], P('dp', 'ctx', 'tp'), may hold values from -4 to 4
Outputs:
- input_grad: bfloat16 [8, 1024, 8192], P('dp', ('ctx', 'tp'))
- query_grad: bfloat16 [8, 1024, 4096], P('dp', 'ctx', 'tp')
- key_grad: bfloat16 [8, 1024, 4096], P('dp', 'ctx', 'tp')
- gate_grad: float32 [2, 8, 32, 1024], P(None, 'dp', 'tp', 'ctx')
- decay_grad: float32 [2, 32], P(None, 'tp')
The draws below stay inside these ranges and needn't reach their ends.
Inputs may be any that keep to these rules, and one draw needn't show every extreme that they name: `gate_logits`: row 0 holds decay logits, row 1 write-strength logits.
All inputs are finite; a program needn't handle non-finite values.
Results may differ from the reference program's by a relative error of at most 0.015.
Values may be sent and summed in bfloat16 or wider, within the bound.
A program may use at most 64 MiB of HBM per device.

```python
import math
import jax
import jax.numpy as jnp
from jax import lax

D = 8192
HD = 128
HEADS_DEV = 2
SUBLEN = 64
TOK_DEV = 256
LOCAL_HEADS = 32
BATCH_SEQUENCES = 8
BLOCKS = 4
SEQUENCE_TOKENS = 1024


def draw_gate_logits(key, part):
    random_subkeys = jax.random.split(key, 8)
    fast_share = 0.5
    shape_head = (BATCH_SEQUENCES, LOCAL_HEADS, 1)
    is_fast = jax.random.uniform(random_subkeys[0], shape_head) < fast_share
    fast_rate = jnp.exp(jax.random.uniform(random_subkeys[1], shape_head, minval=math.log(0.02), maxval=math.log(0.05)))
    slow_rate = jnp.exp(jax.random.uniform(random_subkeys[2], shape_head, minval=math.log(0.1), maxval=math.log(0.5))) / SEQUENCE_TOKENS
    baseline_rate = jnp.where(is_fast, fast_rate, slow_rate)
    block_scaling = jnp.exp(jax.random.uniform(random_subkeys[3], (BATCH_SEQUENCES, LOCAL_HEADS, SEQUENCE_TOKENS // TOK_DEV, 1), minval=math.log(0.5), maxval=math.log(2.0)))
    block_scaling = jnp.broadcast_to(block_scaling, (BATCH_SEQUENCES, LOCAL_HEADS, SEQUENCE_TOKENS // TOK_DEV, TOK_DEV)).reshape(BATCH_SEQUENCES, LOCAL_HEADS, SEQUENCE_TOKENS)
    jaggedness = jnp.exp(jax.random.uniform(random_subkeys[4], (BATCH_SEQUENCES, LOCAL_HEADS, SEQUENCE_TOKENS), minval=math.log(0.5), maxval=math.log(2.0)))
    spike_events = jax.random.uniform(random_subkeys[5], (BATCH_SEQUENCES, LOCAL_HEADS, SEQUENCE_TOKENS)) < 3.0 / SEQUENCE_TOKENS
    spike_rate = jax.random.uniform(random_subkeys[6], (BATCH_SEQUENCES, LOCAL_HEADS, SEQUENCE_TOKENS), minval=0.25, maxval=0.7)
    per_token_rate = baseline_rate * block_scaling * jaggedness + jnp.where(spike_events, spike_rate, 0.0)
    decay_logit = jnp.clip(jnp.log(jnp.expm1(per_token_rate)), -14.0, 1.0)
    strength_logit = jnp.clip(1.5 * jax.random.normal(random_subkeys[7], (BATCH_SEQUENCES, LOCAL_HEADS, SEQUENCE_TOKENS)), -4.0, 4.0)
    return jnp.stack([decay_logit, strength_logit]).astype(jnp.float32)


def block_scale(rng, extent, cuts, least, largest):
    def one(axis_at, shards_of):
        draws = jax.random.uniform(jax.random.fold_in(jax.random.fold_in(rng, 6), axis_at), (shards_of,), jnp.float32, least / len(cuts), largest / len(cuts))
        return jnp.repeat(jnp.exp(draws), extent[axis_at] // shards_of).reshape((-1,) + (1,) * (len(extent) - axis_at - 1))

    loudness = one(*cuts[0])
    for cut in cuts[1:]:
        loudness = loudness * one(*cut)
    return loudness


def centred(own_key, extent, deviation, bound, cuts=(), kind=jnp.bfloat16):
    result = deviation * jax.random.normal(own_key, extent, jnp.float32)
    if cuts:
        result = result * block_scale(own_key, extent, cuts, -0.22, 0.18)
    return jnp.clip(result, -bound, bound).astype(kind)


def setup_inputs(seed: int = 0) -> dict:
    key_of = jax.random.split(jax.random.key(seed), 9)
    layer_input = centred(key_of[0], (BATCH_SEQUENCES, SEQUENCE_TOKENS, D), 1.0, 6.0, ((0, 8), (1, 64)))
    value_weight = centred(key_of[1], (D, LOCAL_HEADS * HD), D ** -0.5, 0.0625, ((0, 32), (1, 16)))
    query_raw = centred(key_of[2], (BATCH_SEQUENCES, SEQUENCE_TOKENS, LOCAL_HEADS * HD), 1.0, 6.0, ((0, 8), (1, 4), (2, 16)))
    key_raw = centred(key_of[3], (BATCH_SEQUENCES, SEQUENCE_TOKENS, LOCAL_HEADS * HD), 1.0, 6.0, ((0, 8), (1, 4), (2, 16)))
    out_grad = centred(key_of[4], (BATCH_SEQUENCES, SEQUENCE_TOKENS, LOCAL_HEADS * HD), 1.0, 6.0, ((0, 8), (1, 4), (2, 16)))
    gate_logits = draw_gate_logits(jax.random.fold_in(key_of[8], 71), 0)
    decay_params = jnp.clip(jax.random.uniform(key_of[6], (2, LOCAL_HEADS), jnp.float32, -0.35, 0.35) * block_scale(key_of[6], (2, LOCAL_HEADS), ((1, 16),), -0.4, 0.0), -0.35, 0.35)
    saved_states = centred(key_of[7], (BATCH_SEQUENCES, BLOCKS, LOCAL_HEADS, HD, HD), 0.5, 4.0, ((0, 8), (1, 4), (2, 16)), jnp.float32)
    return dict(layer_input=layer_input, value_weight=value_weight, query_raw=query_raw, key_raw=key_raw, out_grad=out_grad, gate_logits=gate_logits, decay_params=decay_params, saved_states=saved_states)


epsilon = 1e-06
highest = lax.Precision.HIGHEST

def inner_step(carried, pieces):
    query_unit, key_unit, values, log_decay, strengths = pieces
    sub_len = query_unit.shape[0]
    head_dim = query_unit.shape[1]
    cumulative = jnp.cumsum(log_decay)
    positions = jnp.arange(sub_len)
    lower_mask = positions[:, None] >= positions[None, :]
    strict_mask = positions[:, None] > positions[None, :]
    spread = jnp.where(lower_mask, cumulative[:, None] - cumulative[None, :], 0.0)
    decays = jnp.where(lower_mask, jnp.exp(spread), 0.0)
    key_gram = jnp.dot(key_unit, key_unit.T, precision=highest)
    system = jnp.eye(sub_len, dtype=jnp.float32) + jnp.where(strict_mask, strengths[:, None] * decays * key_gram, 0.0)
    right_side = jnp.concatenate([(strengths * jnp.exp(cumulative))[:, None] * key_unit, strengths[:, None] * values], axis=1)
    solved = jax.scipy.linalg.solve_triangular(system, right_side, lower=True, unit_diagonal=True)
    new_values = solved[:, head_dim:] - jnp.dot(solved[:, :head_dim], carried, precision=highest)
    scores = decays * jnp.dot(query_unit, key_unit.T, precision=highest)
    output = jnp.dot(query_unit * jnp.exp(cumulative)[:, None], carried, precision=highest) + jnp.dot(scores, new_values, precision=highest)
    tail_decay = jnp.exp(cumulative[-1] - cumulative)
    updated = jnp.exp(cumulative[-1]) * carried + jnp.dot((key_unit * tail_decay[:, None]).T, new_values, precision=highest)
    return (updated, output)

def core(query_row, key_row, values, gate_a, gate_b, params, initial):
    length = query_row.shape[0]
    head_dim = query_row.shape[1]
    query_unit = query_row * lax.rsqrt(lax.optimization_barrier(jnp.sum(query_row * query_row, axis=-1, keepdims=True)) + epsilon) * head_dim ** (-0.5)
    key_unit = key_row * lax.rsqrt(lax.optimization_barrier(jnp.sum(key_row * key_row, axis=-1, keepdims=True)) + epsilon)
    log_decay = -jnp.exp(params[0]) * jax.nn.softplus(gate_a + params[1])
    strengths = jax.nn.sigmoid(gate_b)
    blocks = length // SUBLEN

    def into_blocks(array):
        return array.reshape((blocks, SUBLEN) + array.shape[1:])
    final_state, outputs = lax.scan(inner_step, initial, (into_blocks(query_unit), into_blocks(key_unit), into_blocks(values), into_blocks(log_decay), into_blocks(strengths)))
    return (outputs.reshape(length, head_dim), final_state)

def reference(layer_input, value_weight, query_raw, key_raw, out_grad, gate_logits, decay_params, saved_states):
    batch_core = jax.vmap(core, in_axes=(0, 0, 0, 0, 0, None, 0))

    def one_head(head_index):
        columns = lax.dynamic_slice_in_dim(value_weight, head_index * HD, HD, 1)
        value_round = jnp.dot(layer_input.astype(jnp.float32), columns.astype(jnp.float32), preferred_element_type=jnp.float32).astype(jnp.bfloat16)
        value_head = value_round.astype(jnp.float32)
        query_head = lax.dynamic_slice_in_dim(query_raw, head_index * HD, HD, 2).astype(jnp.float32)
        key_head = lax.dynamic_slice_in_dim(key_raw, head_index * HD, HD, 2).astype(jnp.float32)
        grad_head = lax.dynamic_slice_in_dim(out_grad, head_index * HD, HD, 2).astype(jnp.float32)
        gates = lax.dynamic_index_in_dim(gate_logits, head_index, 2, keepdims=False)
        params = lax.dynamic_index_in_dim(decay_params, head_index, 1, keepdims=False)
        states = lax.dynamic_index_in_dim(saved_states, head_index, 2, keepdims=False)
        incoming = jnp.zeros((BATCH_SEQUENCES, HD, HD), jnp.float32)
        param_grad = jnp.zeros((2,), jnp.float32)
        collected = []
        for block_index in reversed(range(BLOCKS)):
            begin = block_index * TOK_DEV
            finish = begin + TOK_DEV
            outputs, pullback = jax.vjp(batch_core, query_head[:, begin:finish], key_head[:, begin:finish], value_head[:, begin:finish], gates[0][:, begin:finish], gates[1][:, begin:finish], params, states[:, block_index])
            gradients = pullback((grad_head[:, begin:finish], incoming))
            incoming = gradients[6]
            param_grad = param_grad + gradients[5]
            collected.append(gradients)
        collected = collected[::-1]
        query_part = jnp.concatenate([part_grads[0] for part_grads in collected], axis=1).astype(jnp.bfloat16)
        key_part = jnp.concatenate([part_grads[1] for part_grads in collected], axis=1).astype(jnp.bfloat16)
        value_part = jnp.concatenate([part_grads[2] for part_grads in collected], axis=1).astype(jnp.bfloat16)
        decay_part = jnp.concatenate([part_grads[3] for part_grads in collected], axis=1)
        strength_part = jnp.concatenate([part_grads[4] for part_grads in collected], axis=1)
        gate_part = jnp.stack([decay_part, strength_part])
        contribution = jnp.einsum('bsc,dc->bsd', value_part.astype(jnp.float32), columns.astype(jnp.float32), precision=highest)
        return (contribution, (query_part, key_part, gate_part, param_grad))

    def one_group(summed_grad, group_index):
        group_sum = jnp.zeros((BATCH_SEQUENCES, SEQUENCE_TOKENS, D), jnp.float32)
        parts = []
        for offset in range(HEADS_DEV):
            contribution, head_parts = one_head(group_index * HEADS_DEV + offset)
            group_sum = group_sum + contribution
            parts.append(head_parts)
        rounded = lax.optimization_barrier(group_sum.astype(jnp.bfloat16))
        summed_grad = summed_grad + rounded.astype(jnp.float32)
        stacked = tuple((jnp.stack([head_parts[index] for head_parts in parts]) for index in range(4)))
        return (summed_grad, stacked)
    summed, per_group = lax.scan(one_group, jnp.zeros((BATCH_SEQUENCES, SEQUENCE_TOKENS, D), jnp.float32), jnp.arange(LOCAL_HEADS // HEADS_DEV, dtype=jnp.int32))
    per_head = tuple((array.reshape((LOCAL_HEADS,) + array.shape[2:]) for array in per_group))
    query_grad = per_head[0].transpose(1, 2, 0, 3).reshape(BATCH_SEQUENCES, SEQUENCE_TOKENS, LOCAL_HEADS * HD)
    key_grad = per_head[1].transpose(1, 2, 0, 3).reshape(BATCH_SEQUENCES, SEQUENCE_TOKENS, LOCAL_HEADS * HD)
    gate_grad = per_head[2].transpose(1, 2, 0, 3)
    decay_grad = per_head[3].T
    return (summed.astype(jnp.bfloat16), query_grad, key_grad, gate_grad, decay_grad)
```

```python
import jax
import jax.numpy as jnp
from jax import lax
from jax.experimental import pallas as pl
from jax.experimental.pallas import tpu as pltpu
from jax.sharding import PartitionSpec as P

f32 = jnp.float32
bf16 = jnp.bfloat16
EPS = 1e-6
MESH = pl.DeviceIdType.MESH

ZN, YN, XN = 8, 8, 4
N, HD, HEADS = 256, 128, 2
TOK = 16
KB = 1024
D = 8192


def mm(a, b, ca=1, cb=0):
    return lax.dot_general(
        a.astype(bf16), b.astype(bf16), (((ca,), (cb,)), ((), ())), preferred_element_type=f32
    )


def exact(a, b):
    return lax.dot_general(
        a, b, (((1,), (0,)), ((), ())), preferred_element_type=f32, precision=lax.Precision.HIGHEST
    )


def softplus(x):
    u = jnp.exp(-jnp.abs(x))
    w = 1.0 + u
    tail = jnp.where(w == 1.0, u, jnp.log(w) * u / jnp.where(w == 1.0, 1.0, w - 1.0))
    return jnp.maximum(x, 0.0) + tail


def sigmoid(x):
    return 1.0 / (1.0 + jnp.exp(-x))


def pair(shape, dim, first, second):
    return jnp.where(lax.broadcasted_iota(jnp.int32, shape, dim) == 0, first, second)


def kernel(
    x_ref, w_ref, q_ref, k_ref, do_ref, gl_ref, par_ref, st_ref,
    ig_ref, qg_ref, kg_ref, gg_ref, dg_ref,
    xs, xg, xl, wg, pcs, pcr, cbs, cbr, dvs, dvg, vp, vr, gl_s, gs, gx, gys, gyr, dct, dzt,
    qn, kn, dec, a_s, p_s, t_s, ef_s, dr_s, s_in,
    xa_s, xa_r, xx_s, xx_r, wp_s, wp_r, wz_s, wz_r, wd_s, wd_r, pc_s, pc_r, cb_s, cb_r,
    dv_s, dv_r, vp_s, vp_r, gx_s, gx_r, gy_s, gy_r, dc_s, dc_r, dz_s, dz_r,
):
    z = lax.axis_index("dp")
    ctx = lax.axis_index("ctx")
    tp = lax.axis_index("tp")
    ylo, c = lax.div(ctx, 2), lax.rem(ctx, 2)
    yhi, x = lax.div(tp, XN), lax.rem(tp, XN)
    yy = yhi * 2 + ylo

    def at(z_, yy_, c_, x_):
        return {
            "dp": z_,
            "ctx": lax.rem(yy_, 2) * 2 + c_,
            "tp": lax.div(yy_, 2) * XN + x_,
        }

    def y_at(o):
        return lax.rem(yy + o, YN)

    def z_at(o):
        return lax.rem(z + o, ZN)

    def x_at(o):
        return lax.rem(x + o, XN)

    def send(src, dst, s, r, device):
        return pltpu.make_async_remote_copy(
            src_ref=src, dst_ref=dst, send_sem=s, recv_sem=r, device_id=device, device_id_type=MESH
        )

    barrier = pltpu.get_barrier_semaphore()
    peers = [at(z, y_at(o), c, x) for o in range(1, YN)]
    peers += [at(z, y_at(o), 1 - c, x) for o in range(YN)]
    peers += [at(z, yy, c, x_at(o)) for o in range(1, XN)]
    peers += [at(z_at(o), yy, c, x) for o in range(1, ZN)]
    for peer in peers:
        pl.semaphore_signal(barrier, inc=1, device_id=peer, device_id_type=MESH)

    for y_ in range(YN):
        for z_ in range(ZN):
            xs[y_, :, z_ * 128 : (z_ + 1) * 128] = x_ref[
                :, z_ * KB + y_ * 128 : z_ * KB + (y_ + 1) * 128
            ]
    xg[x, yy] = xs[yy]
    pl.semaphore_wait(barrier, len(peers))

    to_core = lax.rem(lax.div(yhi, 2) + 1 + lax.div(ctx, 2) + lax.rem(ctx, 2), 2)
    own_half = lax.rem(c + 1 + lax.div(yhi, 2) + lax.rem(yhi, 2), 2)
    w_pre = [
        send(
            w_ref.at[pl.ds(h * 128, 128), :],
            wg.at[lax.div(yhi, 2), z, lax.rem(yhi, 2)],
            wp_s.at[h],
            wp_r.at[lax.rem(yhi, 2)],
            at(z, ctx * 2 + h, to_core, x),
        )
        for h in range(2)
    ]
    w_pre_in = [
        send(w_ref.at[pl.ds(0, 128), :], wg.at[own_half, z, h], wp_s.at[h], wp_r.at[h], at(z, yy, 1 - c, x))
        for h in range(2)
    ]
    for copy in w_pre:
        copy.start()
    x_all = [
        send(xs.at[y_at(o)], xg.at[x, yy], xa_s.at[o], xa_r.at[o], at(z, y_at(o), c, x))
        for o in range(1, YN)
    ]
    for copy in x_all:
        copy.start()

    def w_round():
        for copy in w_pre_in:
            copy.wait_recv()
        for copy in w_sends:
            copy.start()

    w_sends = [
        send(wg.at[own_half, z], wg.at[own_half, z], wz_s.at[o], wz_r.at[o], at(z_at(o), yy, c, x))
        for o in range(1, ZN)
    ]
    x_sends = [
        send(xg.at[x], xg.at[x], xx_s.at[o], xx_r.at[o], at(z, yy, c, x_at(o)))
        for o in range(1, XN)
    ]

    def x_round():
        for copy in x_all:
            copy.wait_recv()
        for copy in x_sends:
            copy.start()

    ii = lax.broadcasted_iota(jnp.int32, (N, N), 0)
    jj = lax.broadcasted_iota(jnp.int32, (N, N), 1)
    low = ii >= jj
    strict = ii > jj
    apart = ii ^ jj
    p0 = pair((HEADS, 1), 0, par_ref[0, 0], par_ref[0, 1])
    p1 = pair((HEADS, 1), 0, par_ref[1, 0], par_ref[1, 1])
    ga = gl_ref[0, 0]
    ld = -jnp.exp(p0) * softplus(ga + p1)
    be = sigmoid(gl_ref[1, 0])
    pad4 = jnp.zeros((4, N), f32)
    upto = jnp.where(ii <= jj, 1.0, 0.0)
    g_rows = exact(jnp.concatenate([ld, be, pad4], axis=0), upto)
    rows = jnp.concatenate([g_rows[:HEADS], be, pad4, jnp.zeros((120, N), f32)], axis=0)
    columns = rows.T
    g_col = [columns[:, h : h + 1] for h in range(HEADS)]
    be_col = [columns[:, HEADS + h : HEADS + h + 1] for h in range(HEADS)]
    gam = [jnp.exp(g) for g in g_col]
    tau = [jnp.exp(g[N - 1 : N, :] - g) for g in g_col]
    gam_n = [jnp.exp(g[N - 1 : N, :]) for g in g_col]

    def head(ref, h):
        return ref[:, h * HD : (h + 1) * HD]

    def inverse_norm(raw):
        return lax.rsqrt(jnp.sum(raw * raw, axis=-1, keepdims=True) + EPS)

    for h in range(HEADS):
        q_raw = head(q_ref, h).astype(f32)
        k_raw = head(k_ref, h).astype(f32)
        qn[h] = q_raw * (inverse_norm(q_raw) * HD**-0.5)
        kn[h] = k_raw * inverse_norm(k_raw)
        dec[h] = jnp.where(low, jnp.exp(jnp.where(low, g_col[h] - g_rows[h : h + 1], 0.0)), 0.0)
        a_s[h] = jnp.where(strict, be_col[h] * dec[h] * mm(kn[h], kn[h], 1, 1), 0.0)
        p_s[h] = dec[h] * mm(qn[h], kn[h], 1, 1)
        t_s[h] = jnp.where(ii == jj, 1.0, jnp.where(apart == 1, -a_s[h], 0.0))
    w_round()

    size = 2
    while size < N:
        for h in range(HEADS):
            level = jnp.where((apart >= size) & (apart < 2 * size), a_s[h], 0.0)
            t_b = t_s[h].astype(bf16)
            t_s[h] = t_s[h] - mm(mm(t_b, level), t_b)
        size *= 2
    x_round()

    for h in range(HEADS):
        do_h = head(do_ref, h)
        start = mm(p_s[h], do_h, 0, 0)
        ef_s[h] = mm(t_s[h], jnp.concatenate([start, kn[h] * tau[h]], axis=1), 0, 0)
        ke = mm(kn[h] * (be_col[h] * gam[h]), ef_s[h], 0, 0)
        const = mm(qn[h] * gam[h], do_h, 0, 0) - ke[:, :HD]
        i2 = lax.broadcasted_iota(jnp.int32, (HD, HD), 0)
        j2 = lax.broadcasted_iota(jnp.int32, (HD, HD), 1)
        carry = jnp.where(i2 == j2, gam_n[h], 0.0) - ke[:, HD:]
        pcs[h] = jnp.concatenate([carry, const], axis=1).astype(bf16)

    to_partner = send(pcs, pcr, pc_s, pc_r, at(z, yy, 1 - c, x))
    to_partner.start()
    to_partner.wait_recv()
    other_y = yy + 1 - 2 * ylo
    even = c == 0
    for h in range(HEADS):
        mine, theirs = pcs[h], pcr[h]
        first = jnp.where(even, mine, theirs)
        last = jnp.where(even, theirs, mine)
        cbs[h] = (mm(first[:, :HD], last[:, HD:]) + first[:, HD:].astype(f32)).astype(bf16)
    to_other = send(cbs, cbr, cb_s, cb_r, at(z, other_y, c, x))
    to_other.start()
    to_other.wait_recv()
    for h in range(HEADS):
        inward = jnp.where(ylo == 0, cbr[h], jnp.zeros((HD, HD), bf16))
        theirs = pcr[h]
        through = mm(theirs[:, :HD], inward) + theirs[:, HD:].astype(f32)
        s_in[h] = jnp.where(even, through, inward.astype(f32))
        dr = ef_s[h][:, :HD] + mm(ef_s[h][:, HD:], s_in[h])
        dr_s[h] = dr
        dvs[:, h * HD : (h + 1) * HD] = (be_col[h] * dr).astype(bf16)
    dv_sends = [
        send(dvs, dvg.at[yy], dv_s.at[o], dv_r.at[o], at(z, y_at(o), c, x)) for o in range(1, YN)
    ]
    for copy in dv_sends:
        copy.start()
    dvg[yy] = dvs[...]

    for copy in w_sends:
        copy.wait_recv()
    w_share = send(wg.at[own_half], wg.at[own_half], wd_s, wd_r, at(z, yy, 1 - c, x))
    w_share.start()
    for copy in x_sends:
        copy.wait_recv()
    for x_ in range(XN):
        for y_ in range(YN):
            row = (y_ % 2) * N + ((y_ // 2) * XN + x_) * TOK
            xl[row : row + TOK, :] = xg[x_, y_]
    w_share.wait_recv()

    def weight(y_hi):
        return wg[lax.div(y_hi, 2), :, lax.rem(y_hi, 2)].reshape(KB, N)

    def v_piece(o, _):
        d = lax.rem(yy + o, YN)
        rows_in = xl[pl.ds(pl.multiple_of(lax.rem(d, 2) * N, N), N), :]
        vp[d] = mm(rows_in, weight(lax.div(d, 2))).astype(bf16)
        return 0

    def v_send(o):
        return send(vp.at[y_at(o)], vr.at[yy], vp_s.at[o], vp_r.at[o], at(z, y_at(o), c, x))

    def v_step(o, _):
        v_piece(o, 0)
        v_send(o).start()
        return 0

    lax.fori_loop(1, YN, v_step, 0)
    v_piece(0, 0)
    vr[yy] = vp[yy]

    for copy in dv_sends:
        copy.wait_recv()

    def g_piece(o):
        x_to = x_at(o)
        for y_ in range(YN):
            row = pl.multiple_of((y_ // 2) * (XN * TOK) + x_to * TOK, TOK)
            for h in range(YN // 2):
                gl_s[y_ * TOK : (y_ + 1) * TOK, h * N : (h + 1) * N] = dvg[
                    h * 2 + y_ % 2, pl.ds(row, TOK), :
                ]
        total = jnp.zeros((YN * TOK, KB), f32)
        for h in range(YN // 2):
            total = total + mm(gl_s[:, h * N : (h + 1) * N], weight(h), 1, 1)
        gs[x_to] = total.astype(bf16)

    def g_send(o):
        return send(gs.at[x_at(o)], gx.at[x], gx_s.at[o], gx_r.at[o], at(z, yy, c, x_at(o)))

    def g_step(o, _):
        g_piece(o)
        g_send(o).start()
        return 0

    lax.fori_loop(1, XN, g_step, 0)
    g_piece(0)
    for o in range(1, XN):
        g_send(o).wait_recv()
    gx[x] = gs[x]
    gys[...] = (
        (gx[0].astype(f32) + gx[1].astype(f32)) + (gx[2].astype(f32) + gx[3].astype(f32))
    ).astype(bf16)
    gy_sends = [
        send(
            gys.at[pl.ds(pl.multiple_of(y_at(o) * TOK, TOK), TOK), :],
            gyr.at[yy], gy_s.at[o], gy_r.at[o], at(z, y_at(o), c, x),
        )
        for o in range(1, YN)
    ]
    for copy in gy_sends:
        copy.start()
    gyr[yy] = gys[pl.ds(pl.multiple_of(yy * TOK, TOK), TOK), :]

    for o in range(1, YN):
        v_send(o).wait_recv()
    values = vr[0].astype(f32)
    for y_ in range(1, YN):
        values = values + vr[y_].astype(f32)
    dvs2 = values.astype(bf16)
    lane = lax.broadcasted_iota(jnp.int32, (N, HD), 1)
    picked = jnp.zeros((N, HD), f32)
    dg_rows = []
    for h in range(HEADS):
        state = st_ref[0, 0, h]
        q_u, k_u = qn[h], kn[h]
        q_b, k_b = q_u.astype(bf16), k_u.astype(bf16)
        d_state, dr = s_in[h], dr_s[h]
        base = dvs2[:, h * HD : (h + 1) * HD].astype(f32) - gam[h] * mm(k_b, state)
        new = mm(t_s[h], be_col[h] * base).astype(bf16)
        do_h = head(do_ref, h)
        both = jnp.concatenate([do_h, dr.astype(bf16)], axis=0)
        cross = mm(both, new, 1, 1)
        by_state = mm(both, state, 1, 1)
        d_p = cross[:N]
        d_a = jnp.where(strict, -cross[N:], 0.0)
        scores = (d_p * dec[h]).astype(bf16)
        gram = (d_a * dec[h] * be_col[h]).astype(bf16)
        da_a = d_a * a_s[h]
        mass = d_p * p_s[h] + da_a
        o_part = gam[h] * by_state[:N]
        r_part = (be_col[h] * gam[h]) * by_state[N:]
        t_part = tau[h] * mm(new, d_state, 1, 1)
        d_q = mm(scores, k_b) + o_part
        d_k = mm(scores, q_b, 0, 0) + mm(gram, k_b) + mm(gram, k_b, 0, 0) - r_part + t_part
        d_be = be_col[h] * jnp.sum(dr * base, axis=1, keepdims=True) + jnp.sum(
            da_a, axis=1, keepdims=True
        )
        tail = jnp.sum(t_part * k_u, axis=1, keepdims=True)
        dg_c = (
            jnp.sum(mass, axis=1, keepdims=True)
            + jnp.sum(o_part * q_u - r_part * k_u, axis=1, keepdims=True)
            - tail
        )
        dg_n = jnp.sum(tail, axis=0, keepdims=True) + gam_n[h] * jnp.sum(
            jnp.sum(state * d_state, axis=1, keepdims=True), axis=0, keepdims=True
        )
        last = lax.broadcasted_iota(jnp.int32, (1, N), 1) == N - 1
        dg_rows.append(jnp.where(last, dg_n, 0.0) - jnp.sum(mass, axis=0, keepdims=True))
        picked = jnp.where(lane == h, dg_c, jnp.where(lane == HEADS + h, d_be, picked))

        def through_norm(d_unit, raw_ref, scale):
            raw = head(raw_ref, h).astype(f32)
            inverse = inverse_norm(raw)
            unit = raw * inverse
            inner = jnp.sum(unit * d_unit, axis=1, keepdims=True)
            return (scale * inverse) * (d_unit - unit * inner)

        qg_ref[0, :, h * HD : (h + 1) * HD] = through_norm(d_q, q_ref, HD**-0.5).astype(bf16)
        kg_ref[0, :, h * HD : (h + 1) * HD] = through_norm(d_k, k_ref, 1.0).astype(bf16)

    picked_rows = picked.T
    dg = picked_rows[:HEADS] + jnp.concatenate(dg_rows, axis=0)
    onward = jnp.where(low, 1.0, 0.0)
    d_ld = exact(jnp.concatenate([dg, jnp.zeros((6, N), f32)], axis=0), onward)[:HEADS]
    d_ga = d_ld * (-jnp.exp(p0)) * sigmoid(ga + p1)
    gg_ref[0, 0] = d_ga
    gg_ref[1, 0] = picked_rows[HEADS : 2 * HEADS] * (1.0 - be)
    scale_sum = jnp.sum(d_ld * ld, axis=1, keepdims=True)
    bias_sum = jnp.sum(d_ga, axis=1, keepdims=True)
    lane2 = lax.broadcasted_iota(jnp.int32, (HEADS, 128), 1)
    mine = jnp.where(lane2 == 0, scale_sum, jnp.where(lane2 == 1, bias_sum, 0.0))
    dct[ctx] = jnp.concatenate([mine, jnp.zeros((6, 128), f32)], axis=0)
    dc_sends = []
    for o, (dy, dc) in enumerate(((0, 1), (1, 0), (1, 1))):
        y_to = yy + dy * (1 - 2 * ylo)
        c_to = c + dc * (1 - 2 * c)
        dc_sends.append(send(dct.at[ctx], dct.at[ctx], dc_s.at[o], dc_r.at[o], at(z, y_to, c_to, x)))
    for copy in dc_sends:
        copy.start()
    for copy in dc_sends:
        copy.wait_recv()
    dzt[z] = (dct[0] + dct[1]) + (dct[2] + dct[3])
    dz_sends = [
        send(dzt.at[z], dzt.at[z], dz_s.at[o], dz_r.at[o], at(z_at(o), yy, c, x))
        for o in range(1, ZN)
    ]
    for copy in dz_sends:
        copy.start()

    for copy in gy_sends:
        copy.wait_recv()
    for y_ in range(YN):
        for z_ in range(ZN):
            ig_ref[0, :, z_ * KB + y_ * 128 : z_ * KB + (y_ + 1) * 128] = gyr[
                y_, :, z_ * 128 : (z_ + 1) * 128
            ]
    for copy in dz_sends:
        copy.wait_recv()
    grand = dzt[0]
    for z_ in range(1, ZN):
        grand = grand + dzt[z_]
    dg_ref[...] = pair(
        (2, 2), 0,
        pair((2, 2), 1, grand[0:1, 0:1], grand[1:2, 0:1]),
        pair((2, 2), 1, grand[0:1, 1:2], grand[1:2, 1:2]),
    )

    for copy in w_pre + x_all + w_sends + x_sends:
        copy.wait_send()
    for copy in [to_partner, to_other, w_share] + dv_sends:
        copy.wait_send()
    for o in range(1, YN):
        v_send(o).wait_send()
    for o in range(1, XN):
        g_send(o).wait_send()
    for copy in gy_sends + dc_sends + dz_sends:
        copy.wait_send()


def per_device(
    layer_input, value_weight, query_raw, key_raw, out_grad, gate_logits, decay_params, saved_states
):
    vmem = pl.BlockSpec(memory_space=pltpu.VMEM)
    dma = pltpu.SemaphoreType.DMA
    V = pltpu.VMEM
    counts = (8, 8, 4, 4, 2, 2, 8, 8, None, None, None, None, None, None)
    counts += (8, 8, 8, 8, 4, 4, 8, 8, 3, 3, 8, 8)
    return pl.pallas_call(
        kernel,
        out_shape=(
            jax.ShapeDtypeStruct((1, TOK, D), bf16),
            jax.ShapeDtypeStruct((1, N, N), bf16),
            jax.ShapeDtypeStruct((1, N, N), bf16),
            jax.ShapeDtypeStruct((2, 1, HEADS, N), f32),
            jax.ShapeDtypeStruct((2, HEADS), f32),
        ),
        in_specs=[vmem] * 6 + [pl.BlockSpec(memory_space=pltpu.SMEM), vmem],
        out_specs=(vmem,) * 5,
        scratch_shapes=[
            V((YN, TOK, KB), bf16),
            V((XN, YN, TOK, KB), bf16),
            V((2 * N, KB), bf16),
            V((2, ZN, 2, 128, N), bf16),
            V((HEADS, HD, 2 * HD), bf16),
            V((HEADS, HD, 2 * HD), bf16),
            V((HEADS, HD, HD), bf16),
            V((HEADS, HD, HD), bf16),
            V((N, N), bf16),
            V((YN, N, N), bf16),
            V((YN, N, N), bf16),
            V((YN, N, N), bf16),
            V((YN * TOK, KB), bf16),
            V((XN, YN * TOK, KB), bf16),
            V((XN, YN * TOK, KB), bf16),
            V((YN * TOK, KB), bf16),
            V((YN, TOK, KB), bf16),
            V((4, 8, 128), f32),
            V((ZN, 8, 128), f32),
            V((HEADS, N, HD), f32),
            V((HEADS, N, HD), f32),
            V((HEADS, N, N), f32),
            V((HEADS, N, N), f32),
            V((HEADS, N, N), f32),
            V((HEADS, N, N), f32),
            V((HEADS, N, 2 * HD), f32),
            V((HEADS, N, HD), f32),
            V((HEADS, HD, HD), f32),
        ]
        + [dma(()) if n is None else dma((n,)) for n in counts],
        compiler_params=pltpu.CompilerParams(
            collective_id=0, has_side_effects=True, vmem_limit_bytes=56 * 2**20
        ),
    )(
        layer_input[0], value_weight, query_raw[0], key_raw[0], out_grad[0],
        gate_logits, decay_params, saved_states,
    )


def solution(mesh):
    placed = (
        P("dp", ("ctx", "tp"), None),
        P(("dp", "ctx"), "tp"),
        P("dp", "ctx", "tp"),
        P("dp", "ctx", "tp"),
        P("dp", "ctx", "tp"),
        P(None, "dp", "tp", "ctx"),
        P(None, "tp"),
        P("dp", "ctx", "tp", None, None),
    )
    return jax.shard_map(
        per_device,
        mesh=mesh,
        in_specs=placed,
        out_specs=(
            P("dp", ("ctx", "tp"), None),
            P("dp", "ctx", "tp"),
            P("dp", "ctx", "tp"),
            P(None, "dp", "tp", "ctx"),
            P(None, "tp"),
        ),
        check_vma=False,
    )
```

```python
import jax
import jax.numpy as jnp
from jax import lax
from jax.experimental import pallas as pl
from jax.experimental.pallas import tpu as pltpu
from jax.sharding import PartitionSpec as P

f32 = jnp.float32
bf16 = jnp.bfloat16
EPS = 1e-6
MESH = pl.DeviceIdType.MESH

ZN, YN, XN = 8, 8, 4
N, HD, HEADS = 256, 128, 2
TOK = 16
KB = 1024
D = 8192


def mm(a, b, ca=1, cb=0):
    return lax.dot_general(
        a.astype(bf16), b.astype(bf16), (((ca,), (cb,)), ((), ())), preferred_element_type=f32
    )


def exact(a, b):
    return lax.dot_general(
        a, b, (((1,), (0,)), ((), ())), preferred_element_type=f32, precision=lax.Precision.HIGHEST
    )


def softplus(x):
    u = jnp.exp(-jnp.abs(x))
    w = 1.0 + u
    tail = jnp.where(w == 1.0, u, jnp.log(w) * u / jnp.where(w == 1.0, 1.0, w - 1.0))
    return jnp.maximum(x, 0.0) + tail


def sigmoid(x):
    return 1.0 / (1.0 + jnp.exp(-x))


def pair(shape, dim, first, second):
    return jnp.where(lax.broadcasted_iota(jnp.int32, shape, dim) == 0, first, second)


def kernel(
    x_ref, w_ref, q_ref, k_ref, do_ref, gl_ref, par_ref, st_ref,
    ig_ref, qg_ref, kg_ref, gg_ref, dg_ref,
    xs, xg, xl, wg, pcs, pcr, cbs, cbr, dvg, vp, vss, vrr, gl_s, gs, gx, gys, gyr, tiles,
    qn, kn, dec, a_s, p_s, t_s, ef_s, dr_s, s_in,
    xa_s, xa_r, xx_s, xx_r, wp_s, wp_r, wz_s, wz_r, wd_s, wd_r, pc_s, pc_r, cb_s, cb_r,
    dv_s, dv_r, vp_s, vp_r, gx_s, gx_r, gy_s, gy_r, dz_s, dz_r,
):
    z = lax.axis_index("dp")
    ctx = lax.axis_index("ctx")
    tp = lax.axis_index("tp")
    ylo, c = lax.div(ctx, 2), lax.rem(ctx, 2)
    yhi, x = lax.div(tp, XN), lax.rem(tp, XN)
    yy = yhi * 2 + ylo

    def at(z_, yy_, c_, x_):
        return {
            "dp": z_,
            "ctx": lax.rem(yy_, 2) * 2 + c_,
            "tp": lax.div(yy_, 2) * XN + x_,
        }

    def y_at(o):
        return lax.rem(yy + o, YN)

    def z_at(o):
        return lax.rem(z + o, ZN)

    def x_at(o):
        return lax.rem(x + o, XN)

    def send(src, dst, s, r, device):
        return pltpu.make_async_remote_copy(
            src_ref=src, dst_ref=dst, send_sem=s, recv_sem=r, device_id=device, device_id_type=MESH
        )

    barrier = pltpu.get_barrier_semaphore()
    peers = [at(z, y_at(o), c, x) for o in range(1, YN)]
    peers += [at(z, y_at(o), 1 - c, x) for o in range(YN)]
    peers += [at(z, yy, c, x_at(o)) for o in range(1, XN)]
    family = [
        (at(z_at(o), yy + dy * (1 - 2 * ylo), c + dc * (1 - 2 * c), x), o, dy, dc)
        for o in range(ZN)
        for dy in range(2)
        for dc in range(2)
        if o + dy + dc > 0
    ]
    peers += [device for device, o, dy, dc in family if o > 0]
    for peer in peers:
        pl.semaphore_signal(barrier, inc=1, device_id=peer, device_id_type=MESH)

    for y_ in range(YN):
        for z_ in range(ZN):
            xs[y_, :, z_ * 128 : (z_ + 1) * 128] = x_ref[
                :, z_ * KB + y_ * 128 : z_ * KB + (y_ + 1) * 128
            ]
    xg[x, yy] = xs[yy]
    ii = lax.broadcasted_iota(jnp.int32, (N, N), 0)
    jj = lax.broadcasted_iota(jnp.int32, (N, N), 1)
    low = ii >= jj
    strict = ii > jj
    apart = ii ^ jj
    p0 = pair((HEADS, 1), 0, par_ref[0, 0], par_ref[0, 1])
    p1 = pair((HEADS, 1), 0, par_ref[1, 0], par_ref[1, 1])
    ga = gl_ref[0, 0]
    ld = -jnp.exp(p0) * softplus(ga + p1)
    be = sigmoid(gl_ref[1, 0])
    pad4 = jnp.zeros((4, N), f32)
    upto = jnp.where(ii <= jj, 1.0, 0.0)
    g_rows = exact(jnp.concatenate([ld, be, pad4], axis=0), upto)
    rows = jnp.concatenate([g_rows[:HEADS], be, pad4, jnp.zeros((120, N), f32)], axis=0)
    columns = rows.T
    g_col = [columns[:, h : h + 1] for h in range(HEADS)]
    be_col = [columns[:, HEADS + h : HEADS + h + 1] for h in range(HEADS)]
    gam = [jnp.exp(g) for g in g_col]
    tau = [jnp.exp(g[N - 1 : N, :] - g) for g in g_col]
    gam_n = [jnp.exp(g[N - 1 : N, :]) for g in g_col]

    def head(ref, h):
        return ref[:, h * HD : (h + 1) * HD]

    def inverse_norm(raw):
        return lax.rsqrt(jnp.sum(raw * raw, axis=-1, keepdims=True) + EPS)

    for h in range(HEADS):
        q_raw = head(q_ref, h).astype(f32)
        k_raw = head(k_ref, h).astype(f32)
        qn[h] = q_raw * (inverse_norm(q_raw) * HD**-0.5)
        kn[h] = k_raw * inverse_norm(k_raw)
        dec[h] = jnp.where(low, jnp.exp(jnp.where(low, g_col[h] - g_rows[h : h + 1], 0.0)), 0.0)
        a_s[h] = jnp.where(strict, be_col[h] * dec[h] * mm(kn[h], kn[h], 1, 1), 0.0)
        p_s[h] = dec[h] * mm(qn[h], kn[h], 1, 1)
        t_s[h] = jnp.where(ii == jj, 1.0, jnp.where(apart == 1, -a_s[h], 0.0))
    size = 2
    while size < N:
        for h in range(HEADS):
            level = jnp.where((apart >= size) & (apart < 2 * size), a_s[h], 0.0)
            t_b = t_s[h].astype(bf16)
            t_s[h] = t_s[h] - mm(mm(t_b, level), t_b)
        size *= 2
    for h in range(HEADS):
        do_h = head(do_ref, h)
        start = mm(p_s[h], do_h, 0, 0)
        ef_s[h] = mm(t_s[h], jnp.concatenate([start, kn[h] * tau[h]], axis=1), 0, 0)
        ke = mm(kn[h] * (be_col[h] * gam[h]), ef_s[h], 0, 0)
        const = mm(qn[h] * gam[h], do_h, 0, 0) - ke[:, :HD]
        i2 = lax.broadcasted_iota(jnp.int32, (HD, HD), 0)
        j2 = lax.broadcasted_iota(jnp.int32, (HD, HD), 1)
        carry = jnp.where(i2 == j2, gam_n[h], 0.0) - ke[:, HD:]
        pcs[h] = jnp.concatenate([carry, const], axis=1).astype(bf16)

    pl.semaphore_wait(barrier, len(peers))

    to_partner = send(pcs, pcr, pc_s, pc_r, at(z, yy, 1 - c, x))
    to_partner.start()
    to_core = lax.rem(lax.div(yhi, 2) + 1 + lax.div(ctx, 2) + lax.rem(ctx, 2), 2)
    own_half = lax.rem(c + 1 + lax.div(yhi, 2) + lax.rem(yhi, 2), 2)
    w_pre = [
        send(
            w_ref.at[pl.ds(h * 128, 128), :],
            wg.at[lax.div(yhi, 2), z, lax.rem(yhi, 2)],
            wp_s.at[h],
            wp_r.at[lax.rem(yhi, 2)],
            at(z, ctx * 2 + h, to_core, x),
        )
        for h in range(2)
    ]
    w_pre_in = [
        send(w_ref.at[pl.ds(0, 128), :], wg.at[own_half, z, h], wp_s.at[h], wp_r.at[h], at(z, yy, 1 - c, x))
        for h in range(2)
    ]
    for copy in w_pre:
        copy.start()
    to_partner.wait_recv()
    other_y = yy + 1 - 2 * ylo
    even = c == 0
    for h in range(HEADS):
        mine, theirs = pcs[h], pcr[h]
        first = jnp.where(even, mine, theirs)
        last = jnp.where(even, theirs, mine)
        cbs[h] = (mm(first[:, :HD], last[:, HD:]) + first[:, HD:].astype(f32)).astype(bf16)
    to_other = send(cbs, cbr, cb_s, cb_r, at(z, other_y, c, x))
    to_other.start()
    x_all = [
        send(xs.at[y_at(o)], xg.at[x, yy], xa_s.at[o], xa_r.at[o], at(z, y_at(o), c, x))
        for o in range(1, YN)
    ]
    for copy in x_all:
        copy.start()

    def z_hop(way, k, half):
        slot = wg.at[own_half, z_at(ZN - k if way == 0 else k), half]
        return send(
            slot, slot, wz_s.at[way, k, half], wz_r.at[way, k, half],
            at(z_at(1 if way == 0 else ZN - 1), yy, c, x),
        )

    def z_arrival(way, k, half):
        slot = wg.at[own_half, z_at(ZN - 1 - k if way == 0 else k + 1), half]
        return send(
            slot, slot, wz_s.at[way, k, half], wz_r.at[way, k, half],
            at(z_at(1 if way == 0 else ZN - 1), yy, c, x),
        )

    def y_hop(way, k, half):
        slot = dvg.at[y_at(YN - k if way == 0 else k), pl.ds(half * 128, 128), :]
        return send(
            slot, slot, dv_s.at[way, k, half], dv_r.at[way, k, half],
            at(z, y_at(1 if way == 0 else YN - 1), c, x),
        )

    def y_arrival(way, k, half):
        slot = dvg.at[y_at(YN - 1 - k if way == 0 else k + 1), pl.ds(half * 128, 128), :]
        return send(
            slot, slot, dv_s.at[way, k, half], dv_r.at[way, k, half],
            at(z, y_at(1 if way == 0 else YN - 1), c, x),
        )

    ring_sends = []

    def launch(copy):
        copy.start()
        ring_sends.append(copy)

    def relay(hop, arrival, k):
        for turn in range(2):
            for way in range(2):
                half = turn if way == 0 else 1 - turn
                if k == 3 and half != way:
                    continue
                arrival(way, k, half).wait_recv()
                if k < 2 or (k == 2 and half == way):
                    launch(hop(way, k + 1, half))

    def share(o):
        slot = wg.at[own_half, z_at(o)]
        return send(slot, slot, wd_s.at[o], wd_r.at[o], at(z, yy, 1 - c, x))

    def x_forward(o):
        x_all[o - 1].wait_recv()
        slot = xg.at[x, y_at(YN - o)]
        for p in range(1, XN):
            launch(send(slot, slot, xx_s.at[p, o], xx_r.at[p, o], at(z, yy, c, x_at(p))))

    for p in range(1, XN):
        slot = xg.at[x, yy]
        launch(send(slot, slot, xx_s.at[p, 0], xx_r.at[p, 0], at(z, yy, c, x_at(p))))
    for half in range(2):
        w_pre_in[half].wait_recv()
        for way in range(2):
            launch(z_hop(way, 0, half))
    launch(share(0))
    to_other.wait_recv()
    for h in range(HEADS):
        inward = jnp.where(ylo == 0, cbr[h], jnp.zeros((HD, HD), bf16))
        theirs = pcr[h]
        through = mm(theirs[:, :HD], inward) + theirs[:, HD:].astype(f32)
        s_in[h] = jnp.where(even, through, inward.astype(f32))
        dr = ef_s[h][:, :HD] + mm(ef_s[h][:, HD:], s_in[h])
        dr_s[h] = dr
        dvg[yy, :, h * HD : (h + 1) * HD] = (be_col[h] * dr).astype(bf16)
    for half in range(2):
        for way in range(2):
            launch(y_hop(way, 0, half if way == 0 else 1 - half))
    for o in (1, 7, 2, 6):
        x_forward(o)
    relay(z_hop, z_arrival, 0)
    launch(share(1))
    launch(share(7))
    for o in (3, 5, 4):
        x_forward(o)
    relay(y_hop, y_arrival, 0)
    relay(z_hop, z_arrival, 1)
    launch(share(2))
    launch(share(6))
    relay(y_hop, y_arrival, 1)
    relay(z_hop, z_arrival, 2)
    launch(share(3))
    launch(share(5))
    relay(y_hop, y_arrival, 2)
    relay(z_hop, z_arrival, 3)
    launch(share(4))
    for p in range(1, XN):
        for o in range(YN):
            slot = xg.at[x_at(XN - p), y_at(YN - o)]
            send(slot, slot, xx_s.at[p, o], xx_r.at[p, o], at(z, yy, c, x_at(p))).wait_recv()
    for x_ in range(XN):
        for y_ in range(YN):
            row = (y_ % 2) * N + ((y_ // 2) * XN + x_) * TOK
            xl[row : row + TOK, :] = xg[x_, y_]
    for o in range(ZN):
        slot = wg.at[1 - own_half, z_at(o)]
        send(slot, slot, wd_s.at[o], wd_r.at[o], at(z, yy, 1 - c, x)).wait_recv()

    def weight(y_hi):
        return wg[lax.div(y_hi, 2), :, lax.rem(y_hi, 2)].reshape(KB, N)

    def v_piece(o, _):
        d = lax.rem(yy + 4 + (1 - 2 * lax.rem(o, 2)) * lax.div(o + 1, 2), YN)
        rows_in = xl[pl.ds(pl.multiple_of(lax.rem(d, 2) * N, N), N), :]
        vp[d] = mm(rows_in, weight(lax.div(d, 2))).astype(bf16)
        return 0

    def v_hop(way, e):
        if e < 2:
            half = e if way == 0 else 1 - e
            d = y_at(4 - e if way == 0 else 4 + e)
            source = vp.at[d, pl.ds(half * 128, 128), :]
        else:
            source = vss.at[way, e - 2]
        return send(
            source, vrr.at[way, e], vp_s.at[way, e], vp_r.at[way, e],
            at(z, y_at(1 if way == 0 else YN - 1), c, x),
        )

    def v_relay(e):
        for way in range(2):
            v_hop(way, e).wait_recv()
            if e < 5:
                left = 3 - (e + 1) // 2
                half = e % 2 if way == 0 else 1 - e % 2
                d = y_at(left if way == 0 else YN - left)
                own = vp[d, half * 128 : half * 128 + 128, :]
                vss[way, e] = (vrr[way, e].astype(f32) + own.astype(f32)).astype(bf16)
                launch(v_hop(way, e + 2))

    lax.fori_loop(0, 3, v_piece, 0)
    for e in range(2):
        for way in range(2):
            launch(v_hop(way, e))
    lax.fori_loop(3, YN, v_piece, 0)

    relay(y_hop, y_arrival, 3)

    def g_piece(o):
        x_to = x_at(o)
        for y_ in range(YN):
            row = pl.multiple_of((y_ // 2) * (XN * TOK) + x_to * TOK, TOK)
            for h in range(YN // 2):
                gl_s[y_ * TOK : (y_ + 1) * TOK, h * N : (h + 1) * N] = dvg[
                    h * 2 + y_ % 2, pl.ds(row, TOK), :
                ]
        total = jnp.zeros((YN * TOK, KB), f32)
        for h in range(YN // 2):
            total = total + mm(gl_s[:, h * N : (h + 1) * N], weight(h), 1, 1)
        gs[x_to] = total.astype(bf16)

    def g_send(o):
        return send(gs.at[x_at(o)], gx.at[x], gx_s.at[o], gx_r.at[o], at(z, yy, c, x_at(o)))

    g_piece(2)
    launch(g_send(2))
    v_relay(0)
    v_relay(1)
    g_piece(1)
    launch(g_send(1))
    v_relay(2)
    g_piece(3)
    launch(g_send(3))
    v_relay(3)
    g_piece(0)
    gx[x] = gs[x]
    v_relay(4)
    for o in range(1, XN):
        g_send(o).wait_recv()
    gys[...] = (
        (gx[0].astype(f32) + gx[1].astype(f32)) + (gx[2].astype(f32) + gx[3].astype(f32))
    ).astype(bf16)
    gy_sends = [
        send(
            gys.at[pl.ds(pl.multiple_of(y_at(o) * TOK, TOK), TOK), :],
            gyr.at[yy], gy_s.at[o], gy_r.at[o], at(z, y_at(o), c, x),
        )
        for o in range(1, YN)
    ]
    for copy in gy_sends:
        copy.start()
    gyr[yy] = gys[pl.ds(pl.multiple_of(yy * TOK, TOK), TOK), :]

    v_relay(5)
    v_relay(6)
    halves = []
    for half in range(2):
        ways = vrr[0, 6 - half].astype(f32) + vrr[1, 5 + half].astype(f32)
        halves.append(vp[yy, half * 128 : half * 128 + 128, :].astype(f32) + ways)
    dvs2 = jnp.concatenate(halves, axis=0).astype(bf16)
    lane = lax.broadcasted_iota(jnp.int32, (N, HD), 1)
    picked = jnp.zeros((N, HD), f32)
    dg_rows = []
    for h in range(HEADS):
        state = st_ref[0, 0, h]
        q_u, k_u = qn[h], kn[h]
        q_b, k_b = q_u.astype(bf16), k_u.astype(bf16)
        d_state, dr = s_in[h], dr_s[h]
        base = dvs2[:, h * HD : (h + 1) * HD].astype(f32) - gam[h] * mm(k_b, state)
        new = mm(t_s[h], be_col[h] * base).astype(bf16)
        do_h = head(do_ref, h)
        both = jnp.concatenate([do_h, dr.astype(bf16)], axis=0)
        cross = mm(both, new, 1, 1)
        by_state = mm(both, state, 1, 1)
        d_p = cross[:N]
        d_a = jnp.where(strict, -cross[N:], 0.0)
        scores = (d_p * dec[h]).astype(bf16)
        gram = (d_a * dec[h] * be_col[h]).astype(bf16)
        da_a = d_a * a_s[h]
        mass = d_p * p_s[h] + da_a
        o_part = gam[h] * by_state[:N]
        r_part = (be_col[h] * gam[h]) * by_state[N:]
        t_part = tau[h] * mm(new, d_state, 1, 1)
        d_q = mm(scores, k_b) + o_part
        d_k = mm(scores, q_b, 0, 0) + mm(gram, k_b) + mm(gram, k_b, 0, 0) - r_part + t_part
        d_be = be_col[h] * jnp.sum(dr * base, axis=1, keepdims=True) + jnp.sum(
            da_a, axis=1, keepdims=True
        )
        tail = jnp.sum(t_part * k_u, axis=1, keepdims=True)
        dg_c = (
            jnp.sum(mass, axis=1, keepdims=True)
            + jnp.sum(o_part * q_u - r_part * k_u, axis=1, keepdims=True)
            - tail
        )
        dg_n = jnp.sum(tail, axis=0, keepdims=True) + gam_n[h] * jnp.sum(
            jnp.sum(state * d_state, axis=1, keepdims=True), axis=0, keepdims=True
        )
        last = lax.broadcasted_iota(jnp.int32, (1, N), 1) == N - 1
        dg_rows.append(jnp.where(last, dg_n, 0.0) - jnp.sum(mass, axis=0, keepdims=True))
        picked = jnp.where(lane == h, dg_c, jnp.where(lane == HEADS + h, d_be, picked))

        def through_norm(d_unit, raw_ref, scale):
            raw = head(raw_ref, h).astype(f32)
            inverse = inverse_norm(raw)
            unit = raw * inverse
            inner = jnp.sum(unit * d_unit, axis=1, keepdims=True)
            return (scale * inverse) * (d_unit - unit * inner)

        qg_ref[0, :, h * HD : (h + 1) * HD] = through_norm(d_q, q_ref, HD**-0.5).astype(bf16)
        kg_ref[0, :, h * HD : (h + 1) * HD] = through_norm(d_k, k_ref, 1.0).astype(bf16)

    picked_rows = picked.T
    dg = picked_rows[:HEADS] + jnp.concatenate(dg_rows, axis=0)
    onward = jnp.where(low, 1.0, 0.0)
    d_ld = exact(jnp.concatenate([dg, jnp.zeros((6, N), f32)], axis=0), onward)[:HEADS]
    d_ga = d_ld * (-jnp.exp(p0)) * sigmoid(ga + p1)
    gg_ref[0, 0] = d_ga
    gg_ref[1, 0] = picked_rows[HEADS : 2 * HEADS] * (1.0 - be)
    scale_sum = jnp.sum(d_ld * ld, axis=1, keepdims=True)
    bias_sum = jnp.sum(d_ga, axis=1, keepdims=True)
    lane2 = lax.broadcasted_iota(jnp.int32, (HEADS, 128), 1)
    mine = jnp.where(lane2 == 0, scale_sum, jnp.where(lane2 == 1, bias_sum, 0.0))
    own_tile = z * 4 + ctx
    tiles[own_tile] = jnp.concatenate([mine, jnp.zeros((6, 128), f32)], axis=0)
    tile_sends = []
    for device, o, dy, dc in family:
        number = o * 4 + dy * 2 + dc
        slot = tiles.at[own_tile]
        copy = send(slot, slot, dz_s.at[number], dz_r.at[number], device)
        copy.start()
        tile_sends.append(copy)
    for copy in gy_sends:
        copy.wait_recv()
    for y_ in range(YN):
        for z_ in range(ZN):
            ig_ref[0, :, z_ * KB + y_ * 128 : z_ * KB + (y_ + 1) * 128] = gyr[
                y_, :, z_ * 128 : (z_ + 1) * 128
            ]
    for copy in tile_sends:
        copy.wait_recv()
    grand = tiles[0]
    for tile in range(1, 4 * ZN):
        grand = grand + tiles[tile]
    dg_ref[...] = pair(
        (2, 2), 0,
        pair((2, 2), 1, grand[0:1, 0:1], grand[1:2, 0:1]),
        pair((2, 2), 1, grand[0:1, 1:2], grand[1:2, 1:2]),
    )

    for copy in w_pre + x_all + [to_partner, to_other] + ring_sends + gy_sends + tile_sends:
        copy.wait_send()


def per_device(
    layer_input, value_weight, query_raw, key_raw, out_grad, gate_logits, decay_params, saved_states
):
    vmem = pl.BlockSpec(memory_space=pltpu.VMEM)
    dma = pltpu.SemaphoreType.DMA
    V = pltpu.VMEM
    counts = [(8,), (4, 8), (2,), (2, 4, 2), (8,), (), (), (2, 4, 2), (2, 7), (4,), (8,), (32,)]
    return pl.pallas_call(
        kernel,
        out_shape=(
            jax.ShapeDtypeStruct((1, TOK, D), bf16),
            jax.ShapeDtypeStruct((1, N, N), bf16),
            jax.ShapeDtypeStruct((1, N, N), bf16),
            jax.ShapeDtypeStruct((2, 1, HEADS, N), f32),
            jax.ShapeDtypeStruct((2, HEADS), f32),
        ),
        in_specs=[vmem] * 6 + [pl.BlockSpec(memory_space=pltpu.SMEM), vmem],
        out_specs=(vmem,) * 5,
        scratch_shapes=[
            V((YN, TOK, KB), bf16),
            V((XN, YN, TOK, KB), bf16),
            V((2 * N, KB), bf16),
            V((2, ZN, 2, 128, N), bf16),
            V((HEADS, HD, 2 * HD), bf16),
            V((HEADS, HD, 2 * HD), bf16),
            V((HEADS, HD, HD), bf16),
            V((HEADS, HD, HD), bf16),
            V((YN, N, N), bf16),
            V((YN, N, N), bf16),
            V((2, 5, 128, N), bf16),
            V((2, 7, 128, N), bf16),
            V((YN * TOK, KB), bf16),
            V((XN, YN * TOK, KB), bf16),
            V((XN, YN * TOK, KB), bf16),
            V((YN * TOK, KB), bf16),
            V((YN, TOK, KB), bf16),
            V((4 * ZN, 8, 128), f32),
            V((HEADS, N, HD), f32),
            V((HEADS, N, HD), f32),
            V((HEADS, N, N), f32),
            V((HEADS, N, N), f32),
            V((HEADS, N, N), f32),
            V((HEADS, N, N), f32),
            V((HEADS, N, 2 * HD), f32),
            V((HEADS, N, HD), f32),
            V((HEADS, HD, HD), f32),
        ]
        + [dma(n) for n in counts for _ in range(2)],
        compiler_params=pltpu.CompilerParams(
            collective_id=0, has_side_effects=True, vmem_limit_bytes=56 * 2**20
        ),
    )(
        layer_input[0], value_weight, query_raw[0], key_raw[0], out_grad[0],
        gate_logits, decay_params, saved_states,
    )


def solution(mesh):
    placed = (
        P("dp", ("ctx", "tp"), None),
        P(("dp", "ctx"), "tp"),
        P("dp", "ctx", "tp"),
        P("dp", "ctx", "tp"),
        P("dp", "ctx", "tp"),
        P(None, "dp", "tp", "ctx"),
        P(None, "tp"),
        P("dp", "ctx", "tp", None, None),
    )
    return jax.shard_map(
        per_device,
        mesh=mesh,
        in_specs=placed,
        out_specs=(
            P("dp", ("ctx", "tp"), None),
            P("dp", "ctx", "tp"),
            P("dp", "ctx", "tp"),
            P(None, "dp", "tp", "ctx"),
            P(None, "tp"),
        ),
        check_vma=False,
    )
```
